32 devices in a mesh: fsdp: 4 (over y, x), seq: 8 (over z, core).
Axes of the slice: x: 2, y: 2, z: 4, core: 2. Of those that a mesh axis runs over, the one named last changes fastest.
Arguments:
- image_input: bfloat16 [4, 1024, 1536], P('fsdp', 'seq'), may hold values from -6 to 6
- text_input: bfloat16 [4, 128, 1536], P('fsdp'), may hold values from -6 to 6
- w_qkv: bfloat16 [1536, 3, 2048], P('fsdp'), may hold values from -0.15625 to 0.15625
- query_gain: float32 [128], replicated, may hold values from 1.2 to 2.4
- key_gain: float32 [128], replicated, may hold values from 1.2 to 2.4
- image_cotangent: bfloat16 [4, 1024, 2048], P('fsdp', 'seq'), may hold values from -6 to 6
- text_cotangent: bfloat16 [4, 128, 2048], P('fsdp'), may hold values from -6 to 6
Outputs:
- image_grad: bfloat16 [4, 1024, 1536], P('fsdp', 'seq')
- text_grad: bfloat16 [4, 128, 1536], P('fsdp')
- weight_grad: float32 [1536, 3, 2048], P('fsdp', None, 'seq')
- gain_grad: float32 [2, 128], replicated
The draws below stay inside these ranges and needn't reach their ends.
All inputs are finite; a program needn't handle non-finite values.
Results may differ from the reference program's by a relative error of at most 0.018.
The reference program's roundings to bfloat16 on the way count: a program that leaves them out, or rounds other values in their place, can miss the bound.
Values may be sent and summed in bfloat16 or wider, within the bound.
A program may use at most 192 MiB of HBM per device.

```python
import math
import jax
import jax.numpy as jnp
from jax import lax

D = 1536
HEADS = 16
HEAD = 128
TXT = 128
IMG_DEV = 128
B_DEV = 1
BATCH = 4
IMG = 1024
N_FSDP = 4
N_SEQ = 8


def steps_of(own_key, dims, cuts, smallest, high):
    factor_of, own = 1.0, jax.random.fold_in(own_key, 6)
    for dim, shards_of in cuts:
        steps = jnp.exp(jax.random.uniform(jax.random.fold_in(own, dim), (shards_of,), jnp.float32, smallest / len(cuts), high / len(cuts)))
        factor_of = factor_of * jnp.repeat(steps, dims[dim] // shards_of).reshape([-1 if axis == dim else 1 for axis in range(len(dims))])
    return factor_of


def gaussian(rng, shape, scale, reach, cuts=(), kind=jnp.bfloat16):
    result = jax.random.normal(rng, shape, jnp.float32) * scale
    if len(cuts) > 0:
        result = steps_of(rng, shape, cuts, -0.22, 0.18) * result
    return jnp.clip(result, min=-reach, max=reach).astype(kind)


def setup_inputs(seed: int = 0) -> dict:
    key_list = jax.random.split(jax.random.key(seed), 8)
    image_input = gaussian(key_list[0], (BATCH, IMG, D), 1.0, 6.0, ((0, 4), (1, 8)))
    text_input = gaussian(key_list[1], (BATCH, TXT, D), 1.0, 6.0, ((0, 4),))
    w_qkv = gaussian(key_list[2], (D, 3, HEADS * HEAD), D ** -0.5, 0.15625, ((0, 4),))
    query_gain = jnp.clip(jnp.exp(jax.random.uniform(key_list[3], (HEAD,), jnp.float32, math.log(1.2), math.log(2.4))), 1.2, 2.4)
    key_gain = jnp.clip(jnp.exp(jax.random.uniform(key_list[4], (HEAD,), jnp.float32, math.log(1.2), math.log(2.4))), 1.2, 2.4)
    image_cotangent = gaussian(key_list[5], (BATCH, IMG, HEADS * HEAD), 1.0, 6.0, ((0, 4), (1, 8)))
    text_cotangent = gaussian(key_list[6], (BATCH, TXT, HEADS * HEAD), 1.0, 6.0, ((0, 4),))
    return dict(image_input=image_input, text_input=text_input, w_qkv=w_qkv, query_gain=query_gain, key_gain=key_gain, image_cotangent=image_cotangent, text_cotangent=text_cotangent)


epsilon = 1e-06
query_parts = 4

def rms_forward(values, gain):
    floated = values.astype(jnp.float32)
    inverse = lax.rsqrt(lax.optimization_barrier(jnp.mean(floated * floated, axis=-1, keepdims=True)) + epsilon)
    return (floated, inverse, (floated * inverse * gain).astype(jnp.bfloat16))

def rms_backward(floated, inverse, gain, incoming):
    weighted = incoming * gain
    inner_mean = lax.optimization_barrier(jnp.mean(weighted * floated, axis=-1, keepdims=True))
    grad_input = inverse * weighted - floated * inverse * inverse * inverse * inner_mean
    grad_gain = lax.optimization_barrier(jnp.sum(incoming * floated * inverse, axis=0))
    return (grad_input, grad_gain)

def head_backward(query_rows, key_rows, value_rows, incoming, query_gain, key_gain):
    query_float, query_inverse, query_normed = rms_forward(query_rows, query_gain)
    key_float, key_inverse, key_normed = rms_forward(key_rows, key_gain)
    length = query_rows.shape[0]
    width = query_rows.shape[1]
    block_rows = length // query_parts
    factor = 1.0 / math.sqrt(width)
    query_blocks = query_normed.reshape(query_parts, block_rows, width)
    incoming_blocks = incoming.reshape(query_parts, block_rows, width)

    def visit(carried, pieces):
        key_total, value_total = carried
        query_piece, incoming_piece = pieces
        scores = jnp.dot(query_piece, key_normed.T, preferred_element_type=jnp.float32) * factor
        attention = jax.nn.softmax(scores, axis=-1)
        attention_grad = jnp.dot(incoming_piece, value_rows.T, preferred_element_type=jnp.float32)
        row_dot = lax.optimization_barrier(jnp.sum(attention * attention_grad, axis=-1, keepdims=True))
        score_grad = (attention * (attention_grad - row_dot)).astype(jnp.bfloat16)
        value_total = value_total + jnp.dot(attention.astype(jnp.bfloat16).T, incoming_piece, preferred_element_type=jnp.float32)
        key_total = key_total + jnp.dot(score_grad.T, query_piece, preferred_element_type=jnp.float32) * factor
        query_grad = jnp.dot(score_grad, key_normed, preferred_element_type=jnp.float32) * factor
        return ((key_total, value_total), query_grad)
    zeros_init = jnp.zeros((length, width), jnp.float32)
    (key_total, value_total), query_pieces = lax.scan(visit, (zeros_init, zeros_init), (query_blocks, incoming_blocks))
    query_grad = query_pieces.reshape(length, width)
    query_input_grad, query_gain_grad = rms_backward(query_float, query_inverse, query_gain, query_grad)
    key_input_grad, key_gain_grad = rms_backward(key_float, key_inverse, key_gain, key_total)
    stacked = jnp.stack([query_input_grad, key_input_grad, value_total], axis=1).astype(jnp.bfloat16)
    return (stacked, jnp.stack([query_gain_grad, key_gain_grad], axis=0))

def reference(image_input, text_input, w_qkv, query_gain, key_gain, image_cotangent, text_cotangent):
    tokens = jnp.concatenate([text_input, image_input], axis=1)
    upstream = jnp.concatenate([text_cotangent, image_cotangent], axis=1)
    weights = w_qkv.astype(jnp.float32)
    triple = jnp.einsum('btd,dch->btch', tokens.astype(jnp.float32), weights).astype(jnp.bfloat16)
    batch_count = triple.shape[0]
    length = triple.shape[1]
    by_heads = triple.reshape(batch_count, length, 3, HEADS, HEAD).transpose(0, 3, 1, 2, 4).reshape(batch_count * HEADS, length, 3, HEAD)
    incoming_heads = upstream.reshape(batch_count, length, HEADS, HEAD).transpose(0, 2, 1, 3).reshape(batch_count * HEADS, length, HEAD)

    def one_head(pair):
        inputs, incoming = pair
        return head_backward(inputs[:, 0], inputs[:, 1], inputs[:, 2], incoming, query_gain, key_gain)
    all_grads, gain_rows = lax.map(one_head, (by_heads, incoming_heads))
    triple_grad = all_grads.reshape(batch_count, HEADS, length, 3, HEAD).transpose(0, 2, 3, 1, 4).reshape(batch_count, length, 3, HEADS * HEAD)
    gain_grad = lax.optimization_barrier(jnp.sum(gain_rows, axis=0))
    full_grad = jnp.einsum('btch,dch->btd', triple_grad.astype(jnp.float32), weights).astype(jnp.bfloat16)
    text_grad = full_grad[:, :TXT]
    image_grad = full_grad[:, TXT:]
    head_group = jnp.arange(HEADS * HEAD, dtype=jnp.int32) // (HEAD * (HEADS // N_SEQ))
    zero_index = jnp.zeros((), jnp.int32)

    def over_groups(group_index, running):
        first_row = (group_index * B_DEV).astype(jnp.int32)
        text_block = lax.dynamic_slice_in_dim(text_input, first_row, B_DEV, 0).astype(jnp.float32)
        text_block_grad = lax.dynamic_slice_in_dim(triple_grad[:, :TXT], first_row, B_DEV, 0).astype(jnp.float32)
        text_part = jnp.einsum('btd,btch->dch', text_block, text_block_grad)

        def over_members(member_index, running_inner):
            image_start = (member_index * IMG_DEV).astype(jnp.int32)
            image_block = lax.dynamic_slice(image_input, (first_row, image_start, zero_index), (B_DEV, IMG_DEV, D)).astype(jnp.float32)
            block_grads = lax.dynamic_slice(triple_grad, (first_row, image_start + TXT, zero_index, zero_index), (B_DEV, IMG_DEV, 3, HEADS * HEAD)).astype(jnp.float32)
            column_mask = (head_group == member_index).astype(jnp.float32)
            partial_value = jnp.einsum('btd,btch->dch', image_block, block_grads) + text_part * column_mask
            rounded = lax.optimization_barrier(partial_value.astype(jnp.bfloat16))
            return running_inner + rounded.astype(jnp.float32)
        return lax.fori_loop(0, N_SEQ, over_members, running)
    weight_grad = lax.fori_loop(0, N_FSDP, over_groups, jnp.zeros((D, 3, HEADS * HEAD), jnp.float32))
    return (image_grad, text_grad, weight_grad, gain_grad)
```

```python
import functools
import math

import jax
import jax.numpy as jnp
from jax import lax
from jax.experimental import pallas as pl
from jax.experimental.pallas import tpu as pltpu
from jax.sharding import PartitionSpec as P

EPSILON = 1e-06
MESH = pl.DeviceIdType.MESH
F32 = jnp.float32
BF16 = jnp.bfloat16
NT = (((1,), (1,)), ((), ()))


def kernel(
    nf, ns, image_ref, text_ref, weight_ref, up_ref, text_up_ref, qg_ref, kg_ref,
    image_out, text_out, weight_out, gain_out,
    tokens, weights, ups, triple, grads, qn_s, kn_s, knt_s, dq_s, dk_s, dv_s,
    sib_send, sib_recv, own_part, z_send, z_recv, w_send, w_recv, gain_all, gain_rows, text_half, tokens_t,
    x_send, x_recv, u_send, u_recv, wg_send, wg_recv, sb_send, sb_recv,
    zs_send, zs_recv, ws_send, ws_recv, g_send, g_recv, h_send, h_recv, t_send, t_recv, l_sem,
):
    f = lax.axis_index("fsdp")
    s = lax.axis_index("seq")
    nz = ns // 2
    z = lax.div(s, 2)
    core = lax.rem(s, 2)
    other = 1 - core
    sib = z * 2 + other
    rows = image_ref.shape[0]
    text_rows = text_ref.shape[0]
    parts, w_rows, all_width = weight_ref.shape
    own_width = all_width // ns
    head = qg_ref.shape[1]
    heads = own_width // head
    length = tokens.shape[0]
    piece = text_rows // ns

    def image_at(index, count=1):
        return pl.ds(pl.multiple_of(text_rows + index * rows, rows), count * rows)

    def remote(src, dst, send, recv, target):
        return pltpu.make_async_remote_copy(
            src_ref=src, dst_ref=dst, send_sem=send, recv_sem=recv,
            device_id=target, device_id_type=MESH,
        )

    barrier = pltpu.get_barrier_semaphore()
    for k in range(1, nf):
        pl.semaphore_signal(
            barrier, inc=1, device_id=(lax.rem(f + k, nf), s), device_id_type=MESH
        )
    for k in range(1, ns):
        pl.semaphore_signal(
            barrier, inc=1, device_id=(f, lax.rem(s + k, ns)), device_id_type=MESH
        )
    pl.semaphore_wait(barrier, nf + ns - 2)

    def x_copy(source, target_s, slot):
        return remote(
            image_ref if source is None else tokens.at[image_at(source)],
            tokens.at[image_at(s if source is None else source)],
            x_send.at[slot],
            x_recv.at[s if source is None else source],
            (f, target_s),
        )

    def w_at(index):
        return pl.ds(pl.multiple_of(index * w_rows, w_rows), w_rows)

    def u_at(index):
        return pl.ds(pl.multiple_of(index * own_width, own_width), own_width)

    own_rows = [
        pltpu.make_async_copy(
            weight_ref.at[c, :, u_at(s)],
            weights.at[w_at(f), pl.ds(c * own_width, own_width)],
            l_sem.at[4 + c],
        )
        for c in range(parts)
    ]
    for copy in own_rows:
        copy.start()
    sends = []
    for k in range(1, nz):
        sends.append(x_copy(None, lax.rem(z + k, nz) * 2 + core, k))
    sends.append(x_copy(None, sib, 0))
    for copy in sends:
        copy.start()
    for copy in own_rows:
        copy.wait()
    for k in range(1, nf):
        target = lax.rem(f + k, nf)
        sends.append(
            remote(
                weights.at[w_at(f)], weights.at[w_at(f)], wg_send.at[k], wg_recv.at[f],
                (target, s),
            )
        )
    for k in range(1, ns):
        target = lax.rem(s + k, ns)
        sends.append(
            remote(
                up_ref.at[:, u_at(target)], ups.at[image_at(s)], u_send.at[k], u_recv.at[s],
                (f, target),
            )
        )
    for copy in sends[nz:]:
        copy.start()
    locals_ = [
        pltpu.make_async_copy(image_ref, tokens.at[image_at(s)], l_sem.at[0]),
        pltpu.make_async_copy(text_ref, tokens.at[pl.ds(0, text_rows)], l_sem.at[1]),
        pltpu.make_async_copy(up_ref.at[:, u_at(s)], ups.at[image_at(s)], l_sem.at[2]),
        pltpu.make_async_copy(
            text_up_ref.at[:, u_at(s)], ups.at[pl.ds(0, text_rows)], l_sem.at[3]
        ),
    ]
    for copy in locals_:
        copy.start()
    for copy in locals_:
        copy.wait()
    for k in range(1, nf):
        source = lax.rem(f - k + nf, nf)
        remote(
            weights.at[w_at(f)], weights.at[w_at(source)], wg_send.at[k], wg_recv.at[source], (f, s)
        ).wait_recv()

    def project(at):
        tokens_t[:, at] = tokens[at, :].T
        triple[at, :] = jnp.dot(
            tokens[at, :], weights[...], preferred_element_type=F32
        ).astype(BF16)

    project(pl.ds(0, text_rows))
    forwards = []
    for k in range(nz):
        zt = lax.rem(z - k + nz, nz)
        if k:
            near = zt * 2 + core
            remote(
                image_ref, tokens.at[image_at(near)], x_send.at[k], x_recv.at[near], (f, s)
            ).wait_recv()
            forward = x_copy(near, sib, nz + k)
            forward.start()
            forwards.append(forward)
        far = zt * 2 + other
        remote(
            image_ref, tokens.at[image_at(far)], x_send.at[k], x_recv.at[far], (f, s)
        ).wait_recv()
        project(image_at(zt * 2, 2))
    for k in range(1, ns):
        source = lax.rem(s - k + ns, ns)
        remote(
            up_ref.at[:, u_at(s)], ups.at[image_at(source)], u_send.at[k], u_recv.at[source],
            (f, s),
        ).wait_recv()

    factor = 1.0 / math.sqrt(head)
    query_gain = qg_ref[...]
    key_gain = kg_ref[...]
    block = max(b for b in range(128, 385, 128) if length % b == 0)

    def columns(c, h):
        return pl.ds(c * own_width + h * head, head)

    def inverse_of(values):
        return lax.rsqrt(jnp.mean(values * values, axis=-1, keepdims=True) + EPSILON)

    def rms_backward(values, gain, incoming):
        inverse = inverse_of(values)
        weighted = incoming * gain
        inner = jnp.mean(weighted * values, axis=-1, keepdims=True)
        grad = inverse * weighted - values * (inverse * inverse * inverse * inner)
        return grad, jnp.sum(incoming * values * inverse, axis=0, keepdims=True)

    gain_q = jnp.zeros((1, head), F32)
    gain_k = jnp.zeros((1, head), F32)
    for h in range(heads):
        qf = triple[:, columns(0, h)].astype(F32)
        qn_s[...] = (qf * inverse_of(qf) * query_gain).astype(BF16)
        kf = triple[:, columns(1, h)].astype(F32)
        kn = (kf * inverse_of(kf) * key_gain).astype(BF16)
        kn_s[...] = kn
        knt_s[...] = kn.astype(F32).T.astype(BF16)
        dk_s[...] = jnp.zeros_like(dk_s)
        dv_s[...] = jnp.zeros_like(dv_s)

        def visit(i, carry, h=h):
            at = pl.ds(pl.multiple_of(i * block, block), block)
            queries = qn_s[at, :]
            upstream = ups[at, pl.ds(h * head, head)]
            scores = lax.dot_general(kn_s[...], queries, NT, preferred_element_type=F32)
            p = jnp.exp(scores * factor)
            p = p * (1.0 / jnp.sum(p, axis=0, keepdims=True))
            dp = lax.dot_general(
                triple[:, columns(2, h)], upstream, NT, preferred_element_type=F32
            )
            dot = jnp.sum(p * dp, axis=0, keepdims=True)
            ds = (p * (dp - dot)).astype(BF16)
            dv_s[...] += jnp.dot(p.astype(BF16), upstream, preferred_element_type=F32)
            dk_s[...] += jnp.dot(ds, queries, preferred_element_type=F32)
            dq_s[at, :] = jnp.dot(knt_s[...], ds, preferred_element_type=F32).T * factor
            return carry

        lax.fori_loop(0, length // block, visit, 0)
        dq, part = rms_backward(triple[:, columns(0, h)].astype(F32), query_gain, dq_s[...])
        gain_q += part
        grads[:, columns(0, h)] = dq.astype(BF16)
        dk, part = rms_backward(
            triple[:, columns(1, h)].astype(F32), key_gain, dk_s[...] * factor
        )
        gain_k += part
        grads[:, columns(1, h)] = dk.astype(BF16)
        grads[:, columns(2, h)] = dv_s[...].astype(BF16)

    gain_all[s, 0:1, :] = gain_q
    gain_all[s, 1:2, :] = gain_k
    for k in range(1, ns):
        copy = remote(
            gain_all.at[s], gain_all.at[s], g_send.at[k], g_recv.at[s], (f, lax.rem(s + k, ns))
        )
        copy.start()
        sends.append(copy)

    def text_at(index):
        return pl.ds(pl.multiple_of(index * piece, piece), piece)

    def share(at):
        return lax.dot_general(grads[at, :], weights[...], NT, preferred_element_type=F32)

    text_share = share(pl.ds(0, text_rows)).astype(BF16)
    text_half[...] = text_share
    siblings = []
    for k in range(nz):
        zt = lax.rem(z + k, nz)
        sib_send[k, pl.ds(0, rows), :] = share(image_at(zt * 2 + other)).astype(BF16)
        sib_send[k, pl.ds(rows, piece), :] = text_half[text_at(zt * 2 + other), :]
        copy = remote(
            sib_send.at[k], sib_recv.at[k], sb_send.at[k], sb_recv.at[k], (f, sib)
        )
        copy.start()
        siblings.append(copy)
    crossing = []
    for k in list(range(1, nz)) + [0]:
        zt = lax.rem(z + k, nz)
        mine = share(image_at(zt * 2 + core))
        siblings[k].wait_recv()
        total = mine + sib_recv[k, pl.ds(0, rows), :].astype(F32)
        text_total = text_half[text_at(zt * 2 + core), :].astype(F32) + sib_recv[
            k, pl.ds(rows, piece), :
        ].astype(F32)
        if k:
            z_send[k, pl.ds(0, rows), :] = total.astype(BF16)
            z_send[k, pl.ds(rows, piece), :] = text_total.astype(BF16)
            copy = remote(
                z_send.at[k], z_recv.at[k], zs_send.at[k], zs_recv.at[k], (f, zt * 2 + core)
            )
            copy.start()
            crossing.append(copy)
        else:
            own_part[pl.ds(0, rows), :] = total
            own_part[pl.ds(rows, piece), :] = text_total

    outgoing = []
    for k in list(range(1, nf)) + [0]:
        target = lax.rem(f + k, nf)
        at = pl.ds(pl.multiple_of(target * w_rows, w_rows), w_rows)
        term = jnp.dot(tokens_t[at, :], grads[...], preferred_element_type=F32)
        if k:
            w_send[k] = term.astype(BF16)
            copy = remote(
                w_send.at[k], w_recv.at[k], ws_send.at[k], ws_recv.at[k], (target, s)
            )
            copy.start()
            outgoing.append(copy)
        else:
            rounded = term.astype(BF16).astype(F32)
            for c in range(parts):
                weight_out[c] = rounded[:, c * own_width : (c + 1) * own_width]

    for k in range(1, ns):
        source = lax.rem(s - k + ns, ns)
        remote(
            gain_all.at[source], gain_all.at[source], g_send.at[k], g_recv.at[source], (f, s)
        ).wait_recv()
    gain = gain_all[0]
    for i in range(1, ns):
        gain += gain_all[i]
    gain_rows[f] = gain
    for k in range(1, nf):
        copy = remote(
            gain_rows.at[f], gain_rows.at[f], h_send.at[k], h_recv.at[f], (lax.rem(f + k, nf), s)
        )
        copy.start()
        sends.append(copy)
    for copy in crossing:
        copy.wait_recv()
    total = own_part[...]
    for k in range(1, nz):
        total += z_recv[k].astype(F32)
    image_out[...] = total[:rows].astype(BF16)
    text_out[text_at(s), :] = total[rows:].astype(BF16)
    texts = []
    for k in range(1, ns):
        target = lax.rem(s + k, ns)
        copy = remote(
            text_out.at[text_at(s)], text_out.at[text_at(s)], t_send.at[k], t_recv.at[s],
            (f, target),
        )
        copy.start()
        sends.append(copy)
    for copy in outgoing:
        copy.wait_recv()
    for k in range(1, nf):
        for c in range(parts):
            weight_out[c] += w_recv[k, :, c * own_width : (c + 1) * own_width].astype(F32)
    for k in range(1, nf):
        source = lax.rem(f - k + nf, nf)
        remote(
            gain_rows.at[source], gain_rows.at[source], h_send.at[k], h_recv.at[source], (f, s)
        ).wait_recv()
    gain = gain_rows[0]
    for i in range(1, nf):
        gain += gain_rows[i]
    gain_out[...] = gain
    for k in range(1, ns):
        source = lax.rem(s - k + ns, ns)
        remote(
            text_out.at[text_at(source)], text_out.at[text_at(source)], t_send.at[k],
            t_recv.at[source], (f, s),
        ).wait_recv()
    for copy in sends + forwards + siblings + crossing + outgoing:
        copy.wait_send()


def local(nf, ns, image_input, text_input, w_qkv, query_gain, key_gain, image_up, text_up):
    _, rows, depth = image_input.shape
    text_rows = text_input.shape[1]
    w_rows, three, all_width = w_qkv.shape
    own_width = all_width // ns
    head = query_gain.shape[0]
    length = text_rows + rows * ns
    nz = ns // 2
    width3 = three * own_width
    tall = rows + text_rows // ns
    vmem = pl.BlockSpec(memory_space=pltpu.VMEM)
    hbm = pl.BlockSpec(memory_space=pl.ANY)
    dma = pltpu.SemaphoreType.DMA
    image_grad, text_grad, weight_grad, gain = pl.pallas_call(
        functools.partial(kernel, nf, ns),
        out_shape=(
            jax.ShapeDtypeStruct((rows, depth), BF16),
            jax.ShapeDtypeStruct((text_rows, depth), BF16),
            jax.ShapeDtypeStruct((three, w_rows, own_width), F32),
            jax.ShapeDtypeStruct((8, head), F32),
        ),
        in_specs=[vmem, vmem, hbm, vmem, hbm, vmem, vmem],
        out_specs=(vmem,) * 4,
        scratch_shapes=[
            pltpu.VMEM((length, depth), BF16),
            pltpu.VMEM((depth, width3), BF16),
            pltpu.VMEM((length, own_width), BF16),
            pltpu.VMEM((length, width3), BF16),
            pltpu.VMEM((length, width3), BF16),
            pltpu.VMEM((length, head), BF16),
            pltpu.VMEM((length, head), BF16),
            pltpu.VMEM((head, length), BF16),
            pltpu.VMEM((length, head), F32),
            pltpu.VMEM((length, head), F32),
            pltpu.VMEM((length, head), F32),
            pltpu.VMEM((nz, tall, depth), BF16),
            pltpu.VMEM((nz, tall, depth), BF16),
            pltpu.VMEM((tall, depth), F32),
            pltpu.VMEM((nz, tall, depth), BF16),
            pltpu.VMEM((nz, tall, depth), BF16),
            pltpu.VMEM((nf, w_rows, width3), BF16),
            pltpu.VMEM((nf, w_rows, width3), BF16),
            pltpu.VMEM((ns, 8, head), F32),
            pltpu.VMEM((nf, 8, head), F32),
            pltpu.VMEM((text_rows, depth), BF16),
            pltpu.VMEM((depth, length), BF16),
            dma((2 * nz,)), dma((ns,)),
            dma((ns,)), dma((ns,)),
            dma((nf,)), dma((nf,)),
            dma((nz,)), dma((nz,)),
            dma((nz,)), dma((nz,)),
            dma((nf,)), dma((nf,)),
            dma((ns,)), dma((ns,)),
            dma((nf,)), dma((nf,)),
            dma((ns,)), dma((ns,)),
            dma((4 + three,)),
        ],
        compiler_params=pltpu.CompilerParams(
            collective_id=0, has_side_effects=True, vmem_limit_bytes=60 * 1024 * 1024
        ),
        name="joint_backward",
    )(
        image_input[0], text_input[0], w_qkv.transpose(1, 0, 2), image_up[0], text_up[0],
        query_gain.reshape(1, head), key_gain.reshape(1, head),
    )
    return (
        image_grad[None],
        text_grad[None],
        weight_grad.transpose(1, 0, 2),
        gain[:2],
    )


def solution(mesh):
    return jax.shard_map(
        functools.partial(local, mesh.shape["fsdp"], mesh.shape["seq"]),
        mesh=mesh,
        in_specs=(
            P("fsdp", "seq", None),
            P("fsdp", None, None),
            P("fsdp", None, None),
            P(),
            P(),
            P("fsdp", "seq", None),
            P("fsdp", None, None),
        ),
        out_specs=(P("fsdp", "seq", None), P("fsdp", None, None), P("fsdp", None, "seq"), P()),
        check_vma=False,
    )
```
